32 devices in a mesh: dp: 8 (over z, y), expert: 4 (over x, core).
Axes of the slice: x: 2, y: 2, z: 4, core: 2. Of those that a mesh axis runs over, the one named last changes fastest.
Arguments:
- tokens: bfloat16 [1024, 4096], P('dp'), may hold values from -6 to 6
- expert_ids: int32 [1024, 2], P('dp'), may hold values from 0 to 3, all different within a row; in each aligned block of 128 rows (0 to 127, 128 to 255, ...) at most 96 rows name the same one
- gate_weights: float32 [1024, 2], P('dp'), may hold values from 0.2 to 1
- live_counts: int32 [8], P('dp'), may hold values from 64 to 128, as said below
- w_gate: bfloat16 [4, 4096, 8192], P('expert', None, 'dp'), may hold values from -0.09375 to 0.09375
- w_up: bfloat16 [4, 4096, 8192], P('expert', None, 'dp'), may hold values from -0.09375 to 0.09375
- w_down: bfloat16 [4, 8192, 4096], P('expert', 'dp'), may hold values from -0.0625 to 0.0625
Outputs:
- mixed: bfloat16 [1024, 4096], P('dp')
- total_loads: int32 [4], replicated
The draws below stay inside these ranges and needn't reach their ends.
Inputs may be any that keep to these rules, and one draw needn't show every extreme that they name: `expert_ids`: each token names two different experts. Among the tokens of one rank no expert is named more than 96 times, a bound that some block reaches in some ranks. Rank r's first live_counts[r] tokens are live, the rest are padding. Some rank has all 128 tokens live.
All inputs are finite; a program needn't handle non-finite values.
Results may differ from the reference program's by a relative error of at most 0.017.
Values may be sent and summed in bfloat16 or wider, within the bound.
A program may use at most 128 MiB of HBM per device.

```python
import math
import jax
import jax.numpy as jnp
import numpy as np
from jax import lax

D = 4096
FF = 8192
TOK_DEV = 128
EXPERTS = 4
CAP = 96
RANKS = 8
TOKENS = 1024
N_DP = 8


def draw_live_counts(key, part):
    base = jax.random.fold_in(key, 11)
    first_key, second_key = jax.random.split(base)
    counts = jax.random.randint(first_key, (RANKS,), TOK_DEV // 2, TOK_DEV + 1)
    full_rank = jax.random.randint(second_key, (), 0, RANKS)
    return jnp.where(jnp.arange(RANKS) == full_rank, TOK_DEV, counts).astype(jnp.int32)


def shard_levels(rng, dims, cuts, smallest, high):
    loudness = 1.0
    for axis_at, blocks in cuts:
        draws = jax.random.uniform(jax.random.fold_in(jax.random.fold_in(rng, 6), axis_at), (blocks,), jnp.float32, smallest / len(cuts), high / len(cuts))
        loudness = loudness * jnp.repeat(jnp.exp(draws), dims[axis_at] // blocks).reshape((-1,) + (1,) * (len(dims) - 1 - axis_at))
    return loudness


def shared_out(rng, own, number, rows, count, top, bound, slope):
    ranking = jax.random.permutation(rng, count)
    packed, usual = load_shares(count, rows * top, bound, slope, True), load_shares(count, rows * top, bound, slope, False)
    places = jnp.arange(count)

    def named(sizes, offset_by):
        used = int((sizes > 0).sum())
        fixed = max(1, used // 4)
        passed = fixed + (places - fixed + offset_by * (used - fixed)) % max(1, count - fixed)
        return jnp.zeros((count,), jnp.int32).at[ranking[jnp.where(places < fixed, places, passed)]].set(jnp.asarray(sizes, jnp.int32))

    sizes = jnp.where(number % 4 == 0, named(packed, number // 4), named(usual, number - number // 4 - 1))
    mixed = jax.random.permutation(jax.random.fold_in(own, 3), count)
    donor, receiver = mixed[0:count // 2 * 2:2], mixed[1:count // 2 * 2:2]
    margin = jnp.minimum(sizes[donor] - 1, bound - sizes[receiver]) // 2
    margin = jnp.where((donor == ranking[0]) | (receiver == ranking[0]) | (sizes[receiver] == 0), 0, jnp.maximum(margin, 0))
    passed = jax.random.randint(jax.random.fold_in(own, 4), (count // 2,), 0, 1 << 20) % (margin + 1)
    sizes = sizes.at[donor].add(-passed).at[receiver].add(passed)
    items = jnp.searchsorted(jnp.cumsum(sizes), jnp.arange(rows * top), side="right").astype(jnp.int32)
    grid = items.reshape(top, rows).T
    grid = grid[jax.random.permutation(jax.random.fold_in(own, 1), rows)]
    offset_by = jax.random.randint(jax.random.fold_in(own, 2), (rows, 1), 0, top)
    return jnp.take_along_axis(grid, (jnp.arange(top)[None, :] + offset_by) % top, axis=1)


def load_shares(amount, total, bound, lean, full):
    portions = [(1 << 20) // math.isqrt(standing ** lean) + 1 for standing in range(1, amount + 1)]
    largest = bound if full else min(bound, max(-(-total // amount), total * portions[0] // sum(portions)))
    least = 1 if total - largest >= amount - 1 else 0
    given, spare = [largest] + [least] * (amount - 1), total - largest - least * (amount - 1)
    while spare > 0:
        movable = [i for i in range(1, amount) if given[i] < largest] or [i for i in range(1, amount) if given[i] < bound]
        whole, left = sum([portions[i] for i in movable]), spare
        for i in movable:
            more = min(bound - given[i], max(1, left * portions[i] // whole), spare)
            given[i] = given[i] + more
            spare = spare - more
    return np.array(given)


def gaussian(own_key, extent, width, bound, pieces=(), held_as=jnp.bfloat16):
    result = width * jax.random.normal(own_key, extent, jnp.float32)
    if pieces:
        result = result * shard_levels(own_key, extent, pieces, -0.22, 0.18)
    return jnp.clip(result, -bound, bound).astype(held_as)


def setup_inputs(seed: int = 0) -> dict:
    streams_of = jax.random.split(jax.random.key(seed), 8)
    tokens = gaussian(streams_of[0], (TOKENS, D), 1.0, 6.0, ((0, 8),))
    expert_ids_keys = jax.random.split(jax.random.fold_in(streams_of[1], 1), TOKENS // TOK_DEV)
    expert_ids_turns = jax.random.permutation(jax.random.fold_in(streams_of[1], 3), TOKENS // TOK_DEV)
    expert_ids = jax.vmap(lambda own, number: shared_out(jax.random.fold_in(streams_of[1], 2), own, number, TOK_DEV, EXPERTS, 2, CAP, 2))(expert_ids_keys, expert_ids_turns).reshape((TOKENS, 2))
    gate_weights = jnp.clip(0.2 + 0.8 * jax.random.uniform(streams_of[2], (TOKENS, 2), jnp.float32) ** shard_levels(streams_of[2], (TOKENS, 2), ((0, 8),), -0.2, 0.2), 0.2, 1.0)
    live_counts = draw_live_counts(jax.random.fold_in(streams_of[7], 71), 0)
    w_gate = gaussian(streams_of[4], (EXPERTS, D, FF), D ** -0.5, 0.09375, ((0, 4), (2, 8)))
    w_up = gaussian(streams_of[5], (EXPERTS, D, FF), D ** -0.5, 0.09375, ((0, 4), (2, 8)))
    w_down = gaussian(streams_of[6], (EXPERTS, FF, D), FF ** -0.5, 0.0625, ((0, 4), (1, 8)))
    return {"tokens": tokens, "expert_ids": expert_ids, "gate_weights": gate_weights, "live_counts": live_counts, "w_gate": w_gate, "w_up": w_up, "w_down": w_down}


def plan_routes(expert_ids, live_total, n_experts, capacity):
    row_count = expert_ids.shape[0]
    is_live = jnp.arange(row_count, dtype=jnp.int32) < live_total
    flat_ids = expert_ids.reshape(-1)
    live_pairs = jnp.repeat(is_live, 2)
    one_hot = ((flat_ids[:, None] == jnp.arange(n_experts, dtype=jnp.int32)[None, :]) & live_pairs[:, None]).astype(jnp.int32)
    earlier = jnp.cumsum(one_hot, axis=0) - one_hot
    slot_index = jnp.sum(earlier * one_hot, axis=1)
    targets = jnp.where(live_pairs, flat_ids * capacity + slot_index, -1).astype(jnp.int32)
    return targets.reshape(row_count, 2), jnp.sum(one_hot, axis=0)


def dispatch_rows(tokens, targets, slots_all):
    wanted = targets.reshape(-1)[None, :] == jnp.arange(slots_all, dtype=jnp.int32)[:, None]
    wanted = jnp.any(wanted.reshape(slots_all, -1, 2), axis=2).astype(jnp.bfloat16)
    return jnp.dot(wanted, tokens, preferred_element_type=jnp.float32).astype(jnp.bfloat16)


def combine_rows(results, targets, gate_weights):
    pick_index = jnp.maximum(targets, 0).astype(jnp.int32)
    selected = results[pick_index].astype(jnp.float32)
    weights = jnp.where(targets >= 0, gate_weights, jnp.zeros_like(gate_weights))
    return jnp.sum(weights[:, :, None] * selected, axis=1).astype(jnp.bfloat16)


def reference(tokens, expert_ids, gate_weights, live_counts, w_gate, w_up, w_down):
    tok_blocks = tokens.reshape(RANKS, TOK_DEV, D)
    id_blocks = expert_ids.reshape(RANKS, TOK_DEV, 2)
    gate_blocks = gate_weights.reshape(RANKS, TOK_DEV, 2)
    targets, loads = jax.vmap(lambda ids, live: plan_routes(ids, live, EXPERTS, CAP))(id_blocks, live_counts)
    outbound = jax.vmap(lambda toks, tgt: dispatch_rows(toks, tgt, EXPERTS * CAP))(tok_blocks, targets)
    per_expert = outbound.reshape(RANKS, EXPERTS, CAP, D).transpose(1, 0, 2, 3).reshape(EXPERTS, RANKS * CAP, D)
    shard_width = FF // N_DP

    def run_expert(operands):
        row_block, gate_matrix, up_matrix, down_matrix = operands
        total = jnp.zeros((row_block.shape[0], D), jnp.float32)
        for shard_index in range(N_DP):
            lower = shard_index * shard_width
            gate_act = jnp.dot(row_block, gate_matrix[:, lower:lower + shard_width], preferred_element_type=jnp.float32)
            up_act = jnp.dot(row_block, up_matrix[:, lower:lower + shard_width], preferred_element_type=jnp.float32)
            hidden = (jax.nn.silu(gate_act) * up_act).astype(jnp.bfloat16)
            partial_term = jnp.dot(hidden, down_matrix[lower:lower + shard_width, :], preferred_element_type=jnp.float32).astype(jnp.bfloat16)
            partial_term = lax.optimization_barrier(partial_term)
            total = total + partial_term.astype(jnp.float32)
        return total.astype(jnp.bfloat16)

    results = lax.map(run_expert, (per_expert, w_gate, w_up, w_down))
    returned = results.reshape(EXPERTS, RANKS, CAP, D).transpose(1, 0, 2, 3).reshape(RANKS, EXPERTS * CAP, D)
    mixed = jax.vmap(combine_rows)(returned, targets, gate_blocks).reshape(TOKENS, D)
    return mixed, jnp.sum(loads, axis=0).astype(jnp.int32)
```

```python
import functools

import jax
import jax.numpy as jnp
from jax import lax
from jax.experimental import pallas as pl
from jax.experimental.pallas import tpu as pltpu
from jax.sharding import PartitionSpec as P

MESH = pl.DeviceIdType.MESH
BF16, F32 = jnp.bfloat16, jnp.float32


def routing_weights(expert_ids, gate_weights, live_total, n_experts, my_expert):
    live = (jnp.arange(expert_ids.shape[0], dtype=jnp.int32) < live_total)[:, None]
    mine = (expert_ids == my_expert) & live
    weight = jnp.sum(jnp.where(mine, gate_weights, 0.0), axis=1)
    named = (expert_ids[:, :, None] == jnp.arange(n_experts, dtype=jnp.int32)) & live[:, :, None]
    return weight, jnp.sum(named.astype(jnp.int32), axis=(0, 1))


def general(tokens, expert_ids, gate_weights, live_counts, w_gate, w_up, w_down):
    weight, loads = routing_weights(
        expert_ids, gate_weights, live_counts[0], lax.axis_size("expert"), lax.axis_index("expert")
    )
    rows = lax.all_gather(tokens, "dp", axis=0, tiled=True)
    scale = lax.all_gather(weight, "dp", axis=0, tiled=True)[:, None]
    gate_act = jnp.dot(rows, w_gate[0], preferred_element_type=F32)
    up_act = jnp.dot(rows, w_up[0], preferred_element_type=F32)
    hidden = (jax.nn.silu(gate_act) * up_act * scale).astype(BF16)
    partial = jnp.dot(hidden, w_down[0], preferred_element_type=F32).astype(BF16)
    summed = lax.psum_scatter(partial, "dp", scatter_dimension=0, tiled=True)
    return lax.psum(summed, "expert"), lax.psum(loads, "dp")


def kernel(n_y, n_planes, tokens, meta, w_gate, w_up, w_down, out, meta_out,
           G, M, WG, WU, WD, H, Y, RC, RY0, RX0, RX1, RY1, RZ, OUT, send_sem, recv_sem, local_sem):
    dp, ex = lax.axis_index("dp"), lax.axis_index("expert")
    z, y = dp // n_y, dp % n_y
    x, c = ex // 2, ex % 2
    yo, xo, co = 1 - y, 1 - x, 1 - c
    n_dp = n_y * n_planes
    pieces, rows, width = G.shape[1:]
    half, quarter = pieces // 2, pieces // 4

    def xor(a, k):
        lo, hi = a % 2, a // 2
        lo = lo if k % 2 == 0 else 1 - lo
        hi = hi if k // 2 == 0 else hi + 1 - 2 * (hi % 2)
        return hi * 2 + lo

    plane = [xor(z, k) for k in range(n_planes)]
    y_peer, x_peer, core_peer = (z * n_y + yo, ex), (dp, xo * 2 + c), (dp, x * 2 + co)
    z_peer = [(plane[k] * n_y + y, ex) for k in range(n_planes)]
    me = dp
    rank = [plane[k] * n_y + y for k in range(n_planes)]
    other = [plane[k] * n_y + yo for k in range(n_planes)]
    pair = [pl.ds(plane[k] * n_y, n_y) for k in range(n_planes)]

    peers = [(lax.rem(dp + d, n_dp), ex) for d in range(1, n_dp)] + [x_peer, core_peer]
    barrier = pltpu.get_barrier_semaphore()

    n_local = [0]

    def local(src, dst):
        copy = pltpu.make_async_copy(src, dst, local_sem.at[n_local[0]])
        n_local[0] += 1
        copy.start()
        return copy

    own_loads = [local(tokens.at[:, pl.ds(q * width, width)], G.at[me, q]) for q in range(pieces)]
    own_meta = local(meta, M.at[me])
    weight_loads = [local(w_gate.at[0], WG), local(w_up.at[0], WU), local(w_down.at[0], WD)]

    for a, b in peers:
        pl.semaphore_signal(barrier, inc=1, device_id={"dp": a, "expert": b}, device_id_type=MESH)
    pl.semaphore_wait(barrier, len(peers))

    sent = []

    def send(src, dst, to):
        i = len(sent)
        copy = pltpu.make_async_remote_copy(
            src_ref=src, dst_ref=dst, send_sem=send_sem.at[i], recv_sem=recv_sem.at[i],
            device_id={"dp": to[0], "expert": to[1]}, device_id_type=MESH,
        )
        copy.start()
        sent.append(copy)
        return copy

    def got(*copies):
        for copy in copies:
            copy.wait_recv()

    mine_x = pl.ds(c * half + x * quarter, quarter)
    mine_c, other_c = pl.ds(c * half, half), pl.ds(co * half, half)

    def piece(xh, o):
        return c * half + xh * quarter + o

    for copy in own_loads:
        copy.wait()
    own_meta.wait()

    ZS = [None] + [send(G.at[me, mine_x], G.at[me, mine_x], z_peer[k]) for k in range(1, n_planes)]
    A0 = send(G.at[me, mine_x], G.at[me, mine_x], y_peer)
    metas = [send(M.at[me], M.at[me], (lax.rem(dp + d, n_dp), ex)) for d in range(1, n_dp)]

    def stage_a(k):
        got(ZS[k])
        ref = G.at[rank[k], piece(x, 0)]
        ref1 = G.at[rank[k], piece(x, 1)]
        return send(ref, ref, x_peer), send(ref1, ref1, y_peer)

    def stage_b(k, a):
        got(a[0])
        first = [G.at[rank[k], piece(h, 0)] for h in range(2)]
        b = [send(ref, ref, y_peer) for ref in first]
        got(a[1])
        ref = G.at[pair[k], piece(x, 1)]
        return b + [send(ref, ref, x_peer)]

    def stage_d(k, b):
        got(*b)
        ref = G.at[pair[k], mine_c]
        return send(ref, ref, core_peer)

    h_tile = min(256, WG.shape[1])

    def gate_up(k):
        columns = [jnp.transpose(M[plane[k] * n_y + j])[:, 0:1] for j in range(n_y)]
        scale = jnp.concatenate(columns, axis=0)

        def tile(t, carry):
            cols = pl.ds(pl.multiple_of(t * h_tile, h_tile), h_tile)
            g = jnp.zeros((n_y * rows, h_tile), F32)
            u = jnp.zeros((n_y * rows, h_tile), F32)
            for q in range(pieces):
                block = G[pair[k], q].reshape(n_y * rows, width)
                g += jnp.dot(block, WG[q * width:(q + 1) * width, cols], preferred_element_type=F32)
            for q in range(pieces):
                block = G[pair[k], q].reshape(n_y * rows, width)
                u += jnp.dot(block, WU[q * width:(q + 1) * width, cols], preferred_element_type=F32)
            H[k, :, cols] = (g / (1.0 + jnp.exp(-g)) * u * scale).astype(BF16)
            return carry

        lax.fori_loop(0, WG.shape[1] // h_tile, tile, 0)

    def down(k):
        def tile(q, carry):
            cols = pl.ds(pl.multiple_of(q * width, width), width)
            part = jnp.dot(H[k], WD[:, cols], preferred_element_type=F32).astype(BF16)
            Y[pair[k], q] = part.reshape(n_y, rows, width)
            return carry

        lax.fori_loop(0, pieces, tile, 0)
        return send(Y.at[pair[k], other_c], RC.at[k], core_peer)

    def add(r, q, value):
        Y[r, q] = (Y[r, q].astype(F32) + value.astype(F32)).astype(BF16)

    def reduce_1(k, r0):
        got(r0)
        for j in range(n_y):
            def tile(q, carry):
                add(plane[k] * n_y + j, c * half + q, RC[k, j, q])
                return carry
            lax.fori_loop(0, half, tile, 0)
        to_y = [send(Y.at[other[k], piece(h, 0)], RY0.at[k, h], y_peer) for h in range(2)]
        to_x = send(Y.at[pair[k], piece(xo, 1)], RX1.at[k], x_peer)
        return to_y, to_x

    def reduce_2(k, r1):
        to_y, to_x = r1
        got(*to_y)
        for h in range(2):
            add(rank[k], piece(h, 0), RY0[k, h])
        x0 = send(Y.at[rank[k], piece(xo, 0)], RX0.at[k], x_peer)
        got(to_x)
        for j in range(n_y):
            add(plane[k] * n_y + j, piece(x, 1), RX1[k, j])
        y1 = send(Y.at[other[k], piece(x, 1)], RY1.at[k], y_peer)
        return x0, y1

    def reduce_3(k, r2):
        got(r2[0])
        add(rank[k], piece(x, 0), RX0[k])
        got(r2[1])
        add(rank[k], piece(x, 1), RY1[k])
        if k:
            return send(Y.at[rank[k], mine_x], RZ.at[k - 1], z_peer[k])

    got(A0)
    ref = G.at[other[0], mine_x]
    B0 = send(ref, ref, x_peer)
    A1 = stage_a(1)
    got(B0)
    ref = G.at[other[0], mine_c]
    D0 = send(ref, ref, core_peer)
    B1 = stage_b(1, A1)
    got(D0)
    got(*metas)
    weight_loads[0].wait()
    weight_loads[1].wait()
    gate_up(0)
    A2 = stage_a(2)
    B2 = stage_b(2, A2)
    D1 = stage_d(1, B1)
    A3 = stage_a(3)
    got(D1)
    gate_up(1)
    B3 = stage_b(3, A3)
    D2 = stage_d(2, B2)
    weight_loads[2].wait()
    C1 = down(1)
    got(D2)
    gate_up(2)
    D3 = stage_d(3, B3)
    P1 = reduce_1(1, C1)
    C2 = down(2)
    got(D3)
    gate_up(3)
    P2 = reduce_1(2, C2)
    Q1 = reduce_2(1, P1)
    C3 = down(3)
    C0 = down(0)
    P3 = reduce_1(3, C3)
    F1 = reduce_3(1, Q1)
    Q2 = reduce_2(2, P2)
    P0 = reduce_1(0, C0)
    F2 = reduce_3(2, Q2)
    Q3 = reduce_2(3, P3)
    F3 = reduce_3(3, Q3)
    Q0 = reduce_2(0, P0)
    reduce_3(0, Q0)

    total = M[0]
    for r in range(1, n_dp):
        total = total + M[r]
    meta_out[...] = total

    got(F1, F2, F3)
    to_x = []
    for o in range(quarter):
        value = Y[me, piece(x, o)].astype(F32)
        for k in range(n_planes - 1):
            value = value + RZ[k, o].astype(F32)
        OUT[piece(x, o)] = value.astype(BF16)
        ref = OUT.at[piece(x, o)]
        to_x.append((send(ref, ref, x_peer), send(ref, ref, core_peer)))
    stores = []

    def store(q):
        stores.append(local(OUT.at[q], out.at[:, pl.ds(pl.multiple_of(q * width, width), width)]))

    last = []
    for o in range(quarter):
        store(piece(x, o))
        got(to_x[o][0])
        ref = OUT.at[piece(xo, o)]
        last.append(send(ref, ref, core_peer))
        store(piece(xo, o))
    for o in range(quarter):
        got(to_x[o][1])
        store(co * half + x * quarter + o)
    for o in range(quarter):
        got(last[o])
        store(co * half + xo * quarter + o)
    for copy in stores:
        copy.wait()
    for copy in sent:
        copy.wait_send()


def planned(n_y, n_planes, tokens, expert_ids, gate_weights, live_counts, w_gate, w_up, w_down):
    n_experts = lax.axis_size("expert")
    rows, model = tokens.shape
    hidden = w_gate.shape[2]
    n_dp, pieces = n_y * n_planes, 8
    width, half, quarter = model // pieces, pieces // 2, pieces // 4
    weight, loads = routing_weights(
        expert_ids, gate_weights, live_counts[0], n_experts, lax.axis_index("expert")
    )
    line = jnp.zeros((rows,), F32).at[:n_experts].set(loads.astype(F32))
    meta = jnp.concatenate([weight[None], line[None], jnp.zeros((6, rows), F32)], axis=0)
    hbm = pl.BlockSpec(memory_space=pl.ANY)
    vmem = pl.BlockSpec(memory_space=pltpu.VMEM)
    mixed, totals = pl.pallas_call(
        functools.partial(kernel, n_y, n_planes),
        name="moe",
        out_shape=(jax.ShapeDtypeStruct((rows, model), BF16), jax.ShapeDtypeStruct((8, rows), F32)),
        in_specs=[hbm] * 5,
        out_specs=(hbm, vmem),
        scratch_shapes=[
            pltpu.VMEM((n_dp, pieces, rows, width), BF16),
            pltpu.VMEM((n_dp, 8, rows), F32),
            pltpu.VMEM((model, hidden), BF16),
            pltpu.VMEM((model, hidden), BF16),
            pltpu.VMEM((hidden, model), BF16),
            pltpu.VMEM((n_planes, n_y * rows, hidden), BF16),
            pltpu.VMEM((n_dp, pieces, rows, width), BF16),
            pltpu.VMEM((n_planes, n_y, half, rows, width), BF16),
            pltpu.VMEM((n_planes, 2, rows, width), BF16),
            pltpu.VMEM((n_planes, rows, width), BF16),
            pltpu.VMEM((n_planes, n_y, rows, width), BF16),
            pltpu.VMEM((n_planes, rows, width), BF16),
            pltpu.VMEM((n_planes - 1, quarter, rows, width), BF16),
            pltpu.VMEM((pieces, rows, width), BF16),
            pltpu.SemaphoreType.DMA((96,)),
            pltpu.SemaphoreType.DMA((96,)),
            pltpu.SemaphoreType.DMA((32,)),
        ],
        compiler_params=pltpu.CompilerParams(
            collective_id=0, has_side_effects=True, vmem_limit_bytes=63 * 2**20
        ),
    )(tokens, meta, w_gate, w_up, w_down)
    return mixed, totals[1, :n_experts].astype(jnp.int32)


def solution(mesh):
    n_dp, n_experts = mesh.shape["dp"], mesh.shape["expert"]
    n_x = n_experts // 2
    n_y = n_x
    n_planes = n_dp // n_y
    body = general
    if n_y == 2 and n_planes == 4:
        body = functools.partial(planned, n_y, n_planes)
    placed = (
        P("dp", None),
        P("dp", None),
        P("dp", None),
        P("dp"),
        P("expert", None, "dp"),
        P("expert", None, "dp"),
        P("expert", "dp", None),
    )
    return jax.shard_map(
        body, mesh=mesh, in_specs=placed, out_specs=(P("dp", None), P()), check_vma=False
    )
```

```python
import functools

import jax
import jax.numpy as jnp
from jax import lax
from jax.experimental import pallas as pl
from jax.experimental.pallas import tpu as pltpu
from jax.sharding import PartitionSpec as P

MESH = pl.DeviceIdType.MESH
BF16, F32 = jnp.bfloat16, jnp.float32


ORDER = "B0 A1 B1 D0 A2 D1 B2 g1 A3 h1 g0 D2 d1 B3 g2 P1 h2 d2 D3 P2 g3 Q1 h3 d3 Q2 F1 P3 F2 h0 d0 Q3 P0 F3 Q0 F0"


def routing_weights(expert_ids, gate_weights, live_total, n_experts, my_expert):
    live = (jnp.arange(expert_ids.shape[0], dtype=jnp.int32) < live_total)[:, None]
    mine = (expert_ids == my_expert) & live
    weight = jnp.sum(jnp.where(mine, gate_weights, 0.0), axis=1)
    named = (expert_ids[:, :, None] == jnp.arange(n_experts, dtype=jnp.int32)) & live[:, :, None]
    return weight, jnp.sum(named.astype(jnp.int32), axis=(0, 1))


def general(tokens, expert_ids, gate_weights, live_counts, w_gate, w_up, w_down):
    weight, loads = routing_weights(
        expert_ids, gate_weights, live_counts[0], lax.axis_size("expert"), lax.axis_index("expert")
    )
    rows = lax.all_gather(tokens, "dp", axis=0, tiled=True)
    scale = lax.all_gather(weight, "dp", axis=0, tiled=True)[:, None]
    gate_act = jnp.dot(rows, w_gate[0], preferred_element_type=F32)
    up_act = jnp.dot(rows, w_up[0], preferred_element_type=F32)
    hidden = (jax.nn.silu(gate_act) * up_act * scale).astype(BF16)
    partial = jnp.dot(hidden, w_down[0], preferred_element_type=F32).astype(BF16)
    summed = lax.psum_scatter(partial, "dp", scatter_dimension=0, tiled=True)
    return lax.psum(summed, "expert"), lax.psum(loads, "dp")


def kernel(n_y, n_planes, tokens, meta, w_gate, w_up, w_down, out, meta_out,
           G, M, WG, WU, WD, H, Y, RC, RY0, RX0, RX1, RY1, RZ, OUT, send_sem, recv_sem, local_sem):
    dp, ex = lax.axis_index("dp"), lax.axis_index("expert")
    z, y = dp // n_y, dp % n_y
    x, c = ex // 2, ex % 2
    yo, xo, co = 1 - y, 1 - x, 1 - c
    n_dp = n_y * n_planes
    pieces, rows, width = G.shape[1:]
    half, quarter = pieces // 2, pieces // 4

    def xor(a, k):
        lo, hi = a % 2, a // 2
        lo = lo if k % 2 == 0 else 1 - lo
        hi = hi if k // 2 == 0 else hi + 1 - 2 * (hi % 2)
        return hi * 2 + lo

    plane = [xor(z, k) for k in range(n_planes)]
    y_peer, x_peer, core_peer = (z * n_y + yo, ex), (dp, xo * 2 + c), (dp, x * 2 + co)
    z_peer = [(plane[k] * n_y + y, ex) for k in range(n_planes)]
    me = dp
    rank = [plane[k] * n_y + y for k in range(n_planes)]
    other = [plane[k] * n_y + yo for k in range(n_planes)]
    pair = [pl.ds(plane[k] * n_y, n_y) for k in range(n_planes)]

    peers = [(lax.rem(dp + d, n_dp), ex) for d in range(1, n_dp)] + [x_peer, core_peer]
    barrier = pltpu.get_barrier_semaphore()

    n_local = [0]

    def local(src, dst):
        copy = pltpu.make_async_copy(src, dst, local_sem.at[n_local[0]])
        n_local[0] += 1
        copy.start()
        return copy

    own_loads = [local(tokens.at[:, pl.ds(q * width, width)], G.at[me, q]) for q in range(pieces)]
    own_meta = local(meta, M.at[me])
    weight_loads = [local(w_gate.at[0], WG), local(w_up.at[0], WU), local(w_down.at[0], WD)]

    for a, b in peers:
        pl.semaphore_signal(barrier, inc=1, device_id={"dp": a, "expert": b}, device_id_type=MESH)
    pl.semaphore_wait(barrier, len(peers))

    sent = []

    def send(src, dst, to):
        i = len(sent)
        copy = pltpu.make_async_remote_copy(
            src_ref=src, dst_ref=dst, send_sem=send_sem.at[i], recv_sem=recv_sem.at[i],
            device_id={"dp": to[0], "expert": to[1]}, device_id_type=MESH,
        )
        copy.start()
        sent.append(copy)
        return copy

    def got(*copies):
        for copy in copies:
            copy.wait_recv()

    mine_x = pl.ds(c * half + x * quarter, quarter)
    mine_c, other_c = pl.ds(c * half, half), pl.ds(co * half, half)

    def piece(xh, o):
        return c * half + xh * quarter + o

    for copy in own_loads:
        copy.wait()
    own_meta.wait()

    own = [G.at[me, piece(x, o)] for o in range(quarter)]
    A = {0: [send(ref, ref, y_peer) for ref in own]}
    ZS = {k: [send(ref, ref, z_peer[k]) for ref in own] for k in range(1, n_planes)}
    metas = [send(M.at[me], M.at[me], (lax.rem(dp + d, n_dp), ex)) for d in range(1, n_dp)]

    B, D, C, R1, R2, F = {}, {}, {}, {}, {}, {}

    def stage_a(k):
        sends = []
        for o, to in ((0, x_peer), (1, y_peer)):
            got(ZS[k][o])
            ref = G.at[rank[k], piece(x, o)]
            sends.append(send(ref, ref, to))
        A[k] = sends

    def stage_b(k):
        B[k] = []
        if k == 0:
            for o in range(2):
                got(A[0][o])
                ref = G.at[other[0], piece(x, o)]
                B[0].append(send(ref, ref, x_peer))
            return
        got(A[k][0])
        for h in range(2):
            ref = G.at[rank[k], piece(h, 0)]
            B[k].append(send(ref, ref, y_peer))
        got(A[k][1])
        ref = G.at[pair[k], piece(x, 1)]
        B[k].append(send(ref, ref, x_peer))

    def stage_d(k):
        got(*B[k])
        ref = G.at[pair[k] if k else other[0], mine_c]
        D[k] = send(ref, ref, core_peer)

    any_done, down_done = [], []
    h_tile = min(256, WG.shape[1])

    def gate_up(k, part):
        if part == 0:
            got(D[k])
            if not any_done:
                any_done.append(k)
                got(*metas)
                weight_loads[0].wait()
                weight_loads[1].wait()
        columns = [jnp.transpose(M[plane[k] * n_y + j])[:, 0:1] for j in range(n_y)]
        scale = jnp.concatenate(columns, axis=0)

        def tile(t, carry):
            cols = pl.ds(pl.multiple_of(t * h_tile, h_tile), h_tile)
            g = jnp.zeros((n_y * rows, h_tile), F32)
            u = jnp.zeros((n_y * rows, h_tile), F32)
            for q in range(pieces):
                block = G[pair[k], q].reshape(n_y * rows, width)
                g += jnp.dot(block, WG[q * width:(q + 1) * width, cols], preferred_element_type=F32)
            for q in range(pieces):
                block = G[pair[k], q].reshape(n_y * rows, width)
                u += jnp.dot(block, WU[q * width:(q + 1) * width, cols], preferred_element_type=F32)
            H[k, :, cols] = (g / (1.0 + jnp.exp(-g)) * u * scale).astype(BF16)
            return carry

        steps = WG.shape[1] // h_tile // 2
        lax.fori_loop(part * steps, (part + 1) * steps, tile, 0)

    def down(k):
        if not down_done:
            down_done.append(k)
            weight_loads[2].wait()
        def tile(q, carry):
            cols = pl.ds(pl.multiple_of(q * width, width), width)
            part = jnp.dot(H[k], WD[:, cols], preferred_element_type=F32).astype(BF16)
            Y[pair[k], q] = part.reshape(n_y, rows, width)
            return carry

        lax.fori_loop(0, pieces, tile, 0)
        C[k] = send(Y.at[pair[k], other_c], RC.at[k], core_peer)

    def add(r, q, value):
        Y[r, q] = (Y[r, q].astype(F32) + value.astype(F32)).astype(BF16)

    def reduce_1(k):
        got(C[k])
        for j in range(n_y):
            def tile(q, carry):
                add(plane[k] * n_y + j, c * half + q, RC[k, j, q])
                return carry
            lax.fori_loop(0, half, tile, 0)
        to_y = [send(Y.at[other[k], piece(h, 0)], RY0.at[k, h], y_peer) for h in range(2)]
        to_x = send(Y.at[pair[k], piece(xo, 1)], RX1.at[k], x_peer)
        R1[k] = to_y, to_x

    def reduce_2(k):
        to_y, to_x = R1[k]
        got(*to_y)
        for h in range(2):
            add(rank[k], piece(h, 0), RY0[k, h])
        x0 = send(Y.at[rank[k], piece(xo, 0)], RX0.at[k], x_peer)
        got(to_x)
        for j in range(n_y):
            add(plane[k] * n_y + j, piece(x, 1), RX1[k, j])
        y1 = send(Y.at[other[k], piece(x, 1)], RY1.at[k], y_peer)
        R2[k] = x0, y1

    def reduce_3(k):
        r2 = R2[k]
        got(r2[0])
        add(rank[k], piece(x, 0), RX0[k])
        got(r2[1])
        add(rank[k], piece(x, 1), RY1[k])
        if k:
            F[k] = send(Y.at[rank[k], mine_x], RZ.at[k - 1], z_peer[k])

    units = {
        "A": stage_a, "B": stage_b, "D": stage_d, "g": lambda k: gate_up(k, 0), "h": lambda k: gate_up(k, 1),
        "d": down, "P": reduce_1, "Q": reduce_2, "F": reduce_3,
    }
    for unit in ORDER.split():
        units[unit[0]](int(unit[1]))

    total = M[0]
    for r in range(1, n_dp):
        total = total + M[r]
    meta_out[...] = total

    got(*F.values())
    to_x = []
    for o in range(quarter):
        value = Y[me, piece(x, o)].astype(F32)
        for k in range(n_planes - 1):
            value = value + RZ[k, o].astype(F32)
        OUT[piece(x, o)] = value.astype(BF16)
        ref = OUT.at[piece(x, o)]
        to_x.append((send(ref, ref, x_peer), send(ref, ref, core_peer)))
    stores = []

    def store(q):
        stores.append(local(OUT.at[q], out.at[:, pl.ds(pl.multiple_of(q * width, width), width)]))

    last = []
    for o in range(quarter):
        store(piece(x, o))
        got(to_x[o][0])
        ref = OUT.at[piece(xo, o)]
        last.append(send(ref, ref, core_peer))
        store(piece(xo, o))
    for o in range(quarter):
        got(to_x[o][1])
        store(co * half + x * quarter + o)
    for o in range(quarter):
        got(last[o])
        store(co * half + xo * quarter + o)
    for copy in stores:
        copy.wait()
    for copy in sent:
        copy.wait_send()


def planned(n_y, n_planes, tokens, expert_ids, gate_weights, live_counts, w_gate, w_up, w_down):
    n_experts = lax.axis_size("expert")
    rows, model = tokens.shape
    hidden = w_gate.shape[2]
    n_dp, pieces = n_y * n_planes, 8
    width, half, quarter = model // pieces, pieces // 2, pieces // 4
    weight, loads = routing_weights(
        expert_ids, gate_weights, live_counts[0], n_experts, lax.axis_index("expert")
    )
    line = jnp.zeros((rows,), F32).at[:n_experts].set(loads.astype(F32))
    meta = jnp.concatenate([weight[None], line[None], jnp.zeros((6, rows), F32)], axis=0)
    hbm = pl.BlockSpec(memory_space=pl.ANY)
    vmem = pl.BlockSpec(memory_space=pltpu.VMEM)
    mixed, totals = pl.pallas_call(
        functools.partial(kernel, n_y, n_planes),
        name="moe",
        out_shape=(jax.ShapeDtypeStruct((rows, model), BF16), jax.ShapeDtypeStruct((8, rows), F32)),
        in_specs=[hbm] * 5,
        out_specs=(hbm, vmem),
        scratch_shapes=[
            pltpu.VMEM((n_dp, pieces, rows, width), BF16),
            pltpu.VMEM((n_dp, 8, rows), F32),
            pltpu.VMEM((model, hidden), BF16),
            pltpu.VMEM((model, hidden), BF16),
            pltpu.VMEM((hidden, model), BF16),
            pltpu.VMEM((n_planes, n_y * rows, hidden), BF16),
            pltpu.VMEM((n_dp, pieces, rows, width), BF16),
            pltpu.VMEM((n_planes, n_y, half, rows, width), BF16),
            pltpu.VMEM((n_planes, 2, rows, width), BF16),
            pltpu.VMEM((n_planes, rows, width), BF16),
            pltpu.VMEM((n_planes, n_y, rows, width), BF16),
            pltpu.VMEM((n_planes, rows, width), BF16),
            pltpu.VMEM((n_planes - 1, quarter, rows, width), BF16),
            pltpu.VMEM((pieces, rows, width), BF16),
            pltpu.SemaphoreType.DMA((96,)),
            pltpu.SemaphoreType.DMA((96,)),
            pltpu.SemaphoreType.DMA((32,)),
        ],
        compiler_params=pltpu.CompilerParams(
            collective_id=0, has_side_effects=True, vmem_limit_bytes=63 * 2**20
        ),
    )(tokens, meta, w_gate, w_up, w_down)
    return mixed, totals[1, :n_experts].astype(jnp.int32)


def solution(mesh):
    n_dp, n_experts = mesh.shape["dp"], mesh.shape["expert"]
    n_x = n_experts // 2
    n_y = n_x
    n_planes = n_dp // n_y
    body = general
    if n_y == 2 and n_planes == 4:
        body = functools.partial(planned, n_y, n_planes)
    placed = (
        P("dp", None),
        P("dp", None),
        P("dp", None),
        P("dp"),
        P("expert", None, "dp"),
        P("expert", None, "dp"),
        P("expert", "dp", None),
    )
    return jax.shard_map(
        body, mesh=mesh, in_specs=placed, out_specs=(P("dp", None), P()), check_vma=False
    )
```

```python
import functools

import jax
import jax.numpy as jnp
from jax import lax
from jax.experimental import pallas as pl
from jax.experimental.pallas import tpu as pltpu
from jax.sharding import PartitionSpec as P

MESH = pl.DeviceIdType.MESH
BF16, F32 = jnp.bfloat16, jnp.float32


ORDER = "B0 A1 B1 D0 A2 D1 B2 g1 A3 h1 D2 d1 B3 g2 P1 h2 d2 D3 P2 g0 Q1 R1 g3 h3 d3 F1 Q2 R2 P3 h0 F2 d0 Q3 R3 P0 F3 X0 X1"


def routing_weights(expert_ids, gate_weights, live_total, n_experts, my_expert):
    live = (jnp.arange(expert_ids.shape[0], dtype=jnp.int32) < live_total)[:, None]
    mine = (expert_ids == my_expert) & live
    weight = jnp.sum(jnp.where(mine, gate_weights, 0.0), axis=1)
    named = (expert_ids[:, :, None] == jnp.arange(n_experts, dtype=jnp.int32)) & live[:, :, None]
    return weight, jnp.sum(named.astype(jnp.int32), axis=(0, 1))


def general(tokens, expert_ids, gate_weights, live_counts, w_gate, w_up, w_down):
    weight, loads = routing_weights(
        expert_ids, gate_weights, live_counts[0], lax.axis_size("expert"), lax.axis_index("expert")
    )
    rows = lax.all_gather(tokens, "dp", axis=0, tiled=True)
    scale = lax.all_gather(weight, "dp", axis=0, tiled=True)[:, None]
    gate_act = jnp.dot(rows, w_gate[0], preferred_element_type=F32)
    up_act = jnp.dot(rows, w_up[0], preferred_element_type=F32)
    hidden = (jax.nn.silu(gate_act) * up_act * scale).astype(BF16)
    partial = jnp.dot(hidden, w_down[0], preferred_element_type=F32).astype(BF16)
    summed = lax.psum_scatter(partial, "dp", scatter_dimension=0, tiled=True)
    return lax.psum(summed, "expert"), lax.psum(loads, "dp")


def kernel(n_y, n_planes, tokens, meta, w_gate, w_up, w_down, out, meta_out,
           G, M, WG, WU, WD, H, Y, RC, RY0, RX0, RX1, RY1, RZ, RO, RP, OUT, send_sem, recv_sem, local_sem):
    dp, ex = lax.axis_index("dp"), lax.axis_index("expert")
    z, y = dp // n_y, dp % n_y
    x, c = ex // 2, ex % 2
    yo, xo, co = 1 - y, 1 - x, 1 - c
    n_dp = n_y * n_planes
    pieces, rows, width = G.shape[1:]
    half, quarter = pieces // 2, pieces // 4

    def xor(a, k):
        lo, hi = a % 2, a // 2
        lo = lo if k % 2 == 0 else 1 - lo
        hi = hi if k // 2 == 0 else hi + 1 - 2 * (hi % 2)
        return hi * 2 + lo

    plane = [xor(z, k) for k in range(n_planes)]
    y_peer, x_peer, core_peer = (z * n_y + yo, ex), (dp, xo * 2 + c), (dp, x * 2 + co)
    z_peer = [(plane[k] * n_y + y, ex) for k in range(n_planes)]
    me = dp
    rank = [plane[k] * n_y + y for k in range(n_planes)]
    other = [plane[k] * n_y + yo for k in range(n_planes)]
    pair = [pl.ds(plane[k] * n_y, n_y) for k in range(n_planes)]

    peers = [(lax.rem(dp + d, n_dp), ex) for d in range(1, n_dp)] + [x_peer, core_peer]
    barrier = pltpu.get_barrier_semaphore()

    n_local = [0]

    def local(src, dst):
        copy = pltpu.make_async_copy(src, dst, local_sem.at[n_local[0]])
        n_local[0] += 1
        copy.start()
        return copy

    own_loads = [local(tokens.at[:, pl.ds(q * width, width)], G.at[me, q]) for q in range(pieces)]
    own_meta = local(meta, M.at[me])
    weight_loads = [local(w_gate.at[0], WG), local(w_up.at[0], WU), local(w_down.at[0], WD)]

    for a, b in peers:
        pl.semaphore_signal(barrier, inc=1, device_id={"dp": a, "expert": b}, device_id_type=MESH)
    pl.semaphore_wait(barrier, len(peers))

    sent = []

    def send(src, dst, to):
        i = len(sent)
        copy = pltpu.make_async_remote_copy(
            src_ref=src, dst_ref=dst, send_sem=send_sem.at[i], recv_sem=recv_sem.at[i],
            device_id={"dp": to[0], "expert": to[1]}, device_id_type=MESH,
        )
        copy.start()
        sent.append(copy)
        return copy

    def got(*copies):
        for copy in copies:
            copy.wait_recv()

    mine_x = pl.ds(c * half + x * quarter, quarter)
    mine_c, other_c = pl.ds(c * half, half), pl.ds(co * half, half)

    def piece(xh, o):
        return c * half + xh * quarter + o

    for copy in own_loads:
        copy.wait()
    own_meta.wait()

    own = [G.at[me, piece(x, o)] for o in range(quarter)]
    A = {0: [send(ref, ref, y_peer) for ref in own]}
    ZS = {k: [send(ref, ref, z_peer[k]) for ref in own] for k in range(1, n_planes)}
    metas = [send(M.at[me], M.at[me], (lax.rem(dp + d, n_dp), ex)) for d in range(1, n_dp)]

    B, D, C, R1, R2, F = {}, {}, {}, {}, {}, {}

    def stage_a(k):
        sends = []
        for o, to in ((0, x_peer), (1, y_peer)):
            got(ZS[k][o])
            ref = G.at[rank[k], piece(x, o)]
            sends.append(send(ref, ref, to))
        A[k] = sends

    def stage_b(k):
        B[k] = []
        if k == 0:
            for o in range(2):
                got(A[0][o])
                ref = G.at[other[0], piece(x, o)]
                B[0].append(send(ref, ref, x_peer))
            return
        got(A[k][0])
        for h in range(2):
            ref = G.at[rank[k], piece(h, 0)]
            B[k].append(send(ref, ref, y_peer))
        got(A[k][1])
        ref = G.at[pair[k], piece(x, 1)]
        B[k].append(send(ref, ref, x_peer))

    def stage_d(k):
        got(*B[k])
        ref = G.at[pair[k] if k else other[0], mine_c]
        D[k] = send(ref, ref, core_peer)

    OY, OX = [], []
    any_done, down_done = [], []
    h_tile = min(256, WG.shape[1])

    def gate_up(k, part):
        if part == 0:
            got(D[k])
            if not any_done:
                any_done.append(k)
                got(*metas)
                weight_loads[0].wait()
                weight_loads[1].wait()
        columns = [jnp.transpose(M[plane[k] * n_y + j])[:, 0:1] for j in range(n_y)]
        scale = jnp.concatenate(columns, axis=0)

        def tile(t, carry):
            cols = pl.ds(pl.multiple_of(t * h_tile, h_tile), h_tile)
            g = jnp.zeros((n_y * rows, h_tile), F32)
            u = jnp.zeros((n_y * rows, h_tile), F32)
            for q in range(pieces):
                block = G[pair[k], q].reshape(n_y * rows, width)
                g += jnp.dot(block, WG[q * width:(q + 1) * width, cols], preferred_element_type=F32)
            for q in range(pieces):
                block = G[pair[k], q].reshape(n_y * rows, width)
                u += jnp.dot(block, WU[q * width:(q + 1) * width, cols], preferred_element_type=F32)
            H[k, :, cols] = (g / (1.0 + jnp.exp(-g)) * u * scale).astype(BF16)
            return carry

        steps = WG.shape[1] // h_tile // 2
        lax.fori_loop(part * steps, (part + 1) * steps, tile, 0)

    def down(k):
        if not down_done:
            down_done.append(k)
            weight_loads[2].wait()
        def tile(q, carry):
            cols = pl.ds(pl.multiple_of(q * width, width), width)
            part = jnp.dot(H[k], WD[:, cols], preferred_element_type=F32).astype(BF16)
            Y[pair[k], q] = part.reshape(n_y, rows, width)
            return carry

        lax.fori_loop(0, pieces, tile, 0, unroll=2)
        C[k] = send(Y.at[pair[k], other_c], RC.at[k], core_peer)

    def add(r, q, value):
        Y[r, q] = (Y[r, q].astype(F32) + value.astype(F32)).astype(BF16)

    def reduce_1(k):
        got(C[k])
        for j in range(n_y):
            def tile(q, carry):
                add(plane[k] * n_y + j, c * half + q, RC[k, j, q])
                return carry
            lax.fori_loop(0, half, tile, 0)
        if k == 0:
            for xh in (xo, x):
                for o in range(quarter):
                    OY.append(send(Y.at[other[0], piece(xh, o)], RO.at[len(OY)], y_peer))
            return
        to_y = [send(Y.at[other[k], piece(h, 0)], RY0.at[k, h], y_peer) for h in range(2)]
        to_x = send(Y.at[pair[k], piece(xo, 1)], RX1.at[k], x_peer)
        R1[k] = to_y, to_x

    def reduce_2x(k):
        got(*R1[k][0])
        for h in range(2):
            add(rank[k], piece(h, 0), RY0[k, h])
        R2[k] = [send(Y.at[rank[k], piece(xo, 0)], RX0.at[k], x_peer)]

    def reduce_2y(k):
        got(R1[k][1])
        for j in range(n_y):
            add(plane[k] * n_y + j, piece(x, 1), RX1[k, j])
        R2[k].append(send(Y.at[other[k], piece(x, 1)], RY1.at[k], y_peer))

    def own_x(half_sent):
        xh = (xo, x)[half_sent]
        if half_sent:
            got(*F.values())
        for o in range(quarter):
            got(OY[half_sent * quarter + o])
            value = Y[me, piece(xh, o)].astype(F32) + RO[half_sent * quarter + o].astype(F32)
            if half_sent:
                for k in range(n_planes - 1):
                    value = value + RZ[k, o].astype(F32)
            Y[me, piece(xh, o)] = value.astype(BF16)
            src = Y.at[me, piece(xh, o)]
            OX.append(send(src, RP.at[half_sent * quarter + o], x_peer))

    def reduce_3(k):
        r2 = R2[k]
        got(r2[0])
        add(rank[k], piece(x, 0), RX0[k])
        got(r2[1])
        add(rank[k], piece(x, 1), RY1[k])
        F[k] = send(Y.at[rank[k], mine_x], RZ.at[k - 1], z_peer[k])

    units = {
        "A": stage_a, "B": stage_b, "D": stage_d, "g": lambda k: gate_up(k, 0), "h": lambda k: gate_up(k, 1),
        "d": down, "P": reduce_1, "Q": reduce_2x, "R": reduce_2y, "F": reduce_3,
        "X": own_x,
    }
    for unit in ORDER.split():
        units[unit[0]](int(unit[1]))

    total = M[0]
    for r in range(1, n_dp):
        total = total + M[r]
    meta_out[...] = total

    stores, last = [], []

    def store(q):
        stores.append(local(OUT.at[q], out.at[:, pl.ds(pl.multiple_of(q * width, width), width)]))

    for i in range(2):
        xh = (x, xo)[i]
        for o in range(quarter):
            got(OX[i * quarter + o])
            kept = Y[me, piece(xh, o)].astype(F32) + RP[i * quarter + o].astype(F32)
            OUT[piece(xh, o)] = kept.astype(BF16)
            ref = OUT.at[piece(xh, o)]
            last.append(send(ref, ref, core_peer))
            store(piece(xh, o))
    for i in range(2):
        xh = (x, xo)[i]
        for o in range(quarter):
            got(last[i * quarter + o])
            store(co * half + xh * quarter + o)
    for copy in stores:
        copy.wait()
    for copy in sent:
        copy.wait_send()


def planned(n_y, n_planes, tokens, expert_ids, gate_weights, live_counts, w_gate, w_up, w_down):
    n_experts = lax.axis_size("expert")
    rows, model = tokens.shape
    hidden = w_gate.shape[2]
    n_dp, pieces = n_y * n_planes, 8
    width, half, quarter = model // pieces, pieces // 2, pieces // 4
    weight, loads = routing_weights(
        expert_ids, gate_weights, live_counts[0], n_experts, lax.axis_index("expert")
    )
    line = jnp.zeros((rows,), F32).at[:n_experts].set(loads.astype(F32))
    meta = jnp.concatenate([weight[None], line[None], jnp.zeros((6, rows), F32)], axis=0)
    hbm = pl.BlockSpec(memory_space=pl.ANY)
    vmem = pl.BlockSpec(memory_space=pltpu.VMEM)
    mixed, totals = pl.pallas_call(
        functools.partial(kernel, n_y, n_planes),
        name="moe",
        out_shape=(jax.ShapeDtypeStruct((rows, model), BF16), jax.ShapeDtypeStruct((8, rows), F32)),
        in_specs=[hbm] * 5,
        out_specs=(hbm, vmem),
        scratch_shapes=[
            pltpu.VMEM((n_dp, pieces, rows, width), BF16),
            pltpu.VMEM((n_dp, 8, rows), F32),
            pltpu.VMEM((model, hidden), BF16),
            pltpu.VMEM((model, hidden), BF16),
            pltpu.VMEM((hidden, model), BF16),
            pltpu.VMEM((n_planes, n_y * rows, hidden), BF16),
            pltpu.VMEM((n_dp, pieces, rows, width), BF16),
            pltpu.VMEM((n_planes, n_y, half, rows, width), BF16),
            pltpu.VMEM((n_planes, 2, rows, width), BF16),
            pltpu.VMEM((n_planes, rows, width), BF16),
            pltpu.VMEM((n_planes, n_y, rows, width), BF16),
            pltpu.VMEM((n_planes, rows, width), BF16),
            pltpu.VMEM((n_planes - 1, quarter, rows, width), BF16),
            pltpu.VMEM((half, rows, width), BF16),
            pltpu.VMEM((half, rows, width), BF16),
            pltpu.VMEM((pieces, rows, width), BF16),
            pltpu.SemaphoreType.DMA((96,)),
            pltpu.SemaphoreType.DMA((96,)),
            pltpu.SemaphoreType.DMA((32,)),
        ],
        compiler_params=pltpu.CompilerParams(
            collective_id=0, has_side_effects=True, vmem_limit_bytes=63 * 2**20
        ),
    )(tokens, meta, w_gate, w_up, w_down)
    return mixed, totals[1, :n_experts].astype(jnp.int32)


def solution(mesh):
    n_dp, n_experts = mesh.shape["dp"], mesh.shape["expert"]
    n_x = n_experts // 2
    n_y = n_x
    n_planes = n_dp // n_y
    body = general
    if n_y == 2 and n_planes == 4:
        body = functools.partial(planned, n_y, n_planes)
    placed = (
        P("dp", None),
        P("dp", None),
        P("dp", None),
        P("dp"),
        P("expert", None, "dp"),
        P("expert", None, "dp"),
        P("expert", "dp", None),
    )
    return jax.shard_map(
        body, mesh=mesh, in_specs=placed, out_specs=(P("dp", None), P()), check_vma=False
    )
```
